32 devices in a mesh: flow: 8 (over y, x, core), span: 4 (over z).
Axes of the slice: x: 2, y: 2, z: 4, core: 2. Of those that a mesh axis runs over, the one named last changes fastest.
Arguments:
- solid_start: float32 [32, 512, 512], P(None, 'flow', 'span'), may hold values from -6 to 6
- heat_gen: float32 [32, 512, 512], P(None, 'flow', 'span'), may hold values from 0 to 0.05
- conductance: float32 [64, 16384], P('span', 'flow'), may hold values from 0 to 1, as said below
- heat_capacity: float32 [64], P('span'), may hold values from 0.2 to 1
- inlet_temp: float32 [64], P('span'), may hold values from -4 to 4
- wall_owner: int32 [8192, 1], P(('flow', 'span')), may hold values from 0 to 7; in each aligned block of 256 rows (0 to 255, 256 to 511, ...) at most 64 rows name the same one
- wall_row: int32 [8192, 1], P(('flow', 'span')), may hold values from 0 to 63
Outputs:
- solid_final: float32 [32, 512, 512], P(None, 'flow', 'span')
- coolant_final: float32 [64, 16384], P('span', 'flow')
The draws below stay inside these ranges and needn't reach their ends.
Inputs may be any that keep to these rules, and one draw needn't show every extreme that they name: `conductance`: Positive. `wall_owner`: within the segments of one device (aligned blocks of 256 rows) no flow index is named more than 64 times, and some flow index is named exactly 64 times.
All inputs are finite; a program needn't handle non-finite values.
Results may differ from the reference program's by a relative error of at most 0.0003.
Values sent between devices are 32-bit elements; how exact they have to be, the bound alone decides.
A program may use at most 128 MiB of HBM per device.

```python
import math
import jax
import jax.numpy as jnp
import numpy as np
from jax import lax

SEG = 128
NZ = 32
CX = 64
CH_DEV = 16
ST_DEV = 2048
STEPS = 10
NX = 512
NY = 512
CHANNELS = 64
CHANNEL_STATIONS = 16384
SEG_DEV = 256
SEGS = 8192
CAP = 64
N_FLOW = 8
N_SPAN = 4


def draw_conductance(key, part):
    random_child_keys = jax.random.split(key, 6)
    solid_grid_shape = (CHANNELS, CHANNEL_STATIONS)
    fast_share = 0.5
    fast_mask = jax.random.uniform(random_child_keys[0], (CHANNELS, 1)) < fast_share
    slow_rates = jnp.exp(jax.random.uniform(random_child_keys[1], (CHANNELS, 1), jnp.float32, math.log(5.0), math.log(40.0))) / CHANNEL_STATIONS
    fast_rates = jnp.exp(jax.random.uniform(random_child_keys[2], (CHANNELS, 1), jnp.float32, math.log(1.0 / 50.0), math.log(1.0 / 30.0)))
    decay_rates = jnp.where(fast_mask, fast_rates, slow_rates)
    surface_texture = jax.random.uniform(random_child_keys[3], solid_grid_shape, jnp.float32, 0.5, 1.5)
    surge_event_mask = jax.random.uniform(random_child_keys[4], solid_grid_shape) < 3.0 / CHANNEL_STATIONS
    surge_heat_loss = jax.random.uniform(random_child_keys[5], solid_grid_shape, jnp.float32, 0.2, 0.5)
    sampled_values = jnp.where(surge_event_mask, -jnp.log(1.0 - surge_heat_loss), decay_rates * surface_texture)
    return sampled_values.astype(jnp.float32)


def set_ends(array, rng, low, largest):
    shape = array.shape
    place = [jax.random.randint(jax.random.fold_in(rng, axis), (), 0, shape[axis]) for axis in range(len(shape))]
    array = array.at[tuple(place)].set(low)
    longest = shape.index(max(shape))
    place[longest] = (place[longest] + 1) % shape[longest]
    return array.at[tuple(place)].set(largest)


def block_scale(own_key, extent, cuts, least, top_value):
    gain, own = 1.0, jax.random.fold_in(own_key, 6)
    for axis_at, shards_of in cuts:
        heights = jnp.exp(jax.random.uniform(jax.random.fold_in(own, axis_at), (shards_of,), jnp.float32, least / len(cuts), top_value / len(cuts)))
        gain = gain * jnp.repeat(heights, extent[axis_at] // shards_of).reshape([-1 if axis == axis_at else 1 for axis in range(len(extent))])
    return gain


def deal_out(own_key, own, number, rows, amount, top, reach, skew):
    sequence = jax.random.permutation(own_key, amount)
    crowded, common = portions_of(amount, rows * top, reach, skew, True), portions_of(amount, rows * top, reach, skew, False)
    places = jnp.arange(amount)

    def named(sizes, rotation):
        used = int((sizes > 0).sum())
        fixed = max(1, used // 4)
        shifted = fixed + (places - fixed + rotation * (used - fixed)) % max(1, amount - fixed)
        return jnp.zeros((amount,), jnp.int32).at[sequence[jnp.where(places < fixed, places, shifted)]].set(jnp.asarray(sizes, jnp.int32))

    sizes = jnp.where(number % 4 == 0, named(crowded, number // 4), named(common, number - number // 4 - 1))
    mixed = jax.random.permutation(jax.random.fold_in(own, 3), amount)
    giver, receiver = mixed[0:amount // 2 * 2:2], mixed[1:amount // 2 * 2:2]
    margin = jnp.minimum(sizes[giver] - 1, reach - sizes[receiver]) // 2
    margin = jnp.where((giver == sequence[0]) | (receiver == sequence[0]) | (sizes[receiver] == 0), 0, jnp.maximum(margin, 0))
    shifted = jax.random.randint(jax.random.fold_in(own, 4), (amount // 2,), 0, 1 << 20) % (margin + 1)
    sizes = sizes.at[giver].add(-shifted).at[receiver].add(shifted)
    labels = jnp.searchsorted(jnp.cumsum(sizes), jnp.arange(rows * top), side="right").astype(jnp.int32)
    table = labels.reshape(top, rows).T
    table = table[jax.random.permutation(jax.random.fold_in(own, 1), rows)]
    rotation = jax.random.randint(jax.random.fold_in(own, 2), (rows, 1), 0, top)
    return jnp.take_along_axis(table, (jnp.arange(top)[None, :] + rotation) % top, axis=1)


def portions_of(count, total, most, lean, full):
    portions = [(1 << 20) // math.isqrt(grade ** lean) + 1 for grade in range(1, count + 1)]
    largest = most if full else min(most, max(-(-total // count), total * portions[0] // sum(portions)))
    least = 1 if total - largest >= count - 1 else 0
    given, rest = [largest] + [least] * (count - 1), total - largest - least * (count - 1)
    while rest > 0:
        free = [i for i in range(1, count) if given[i] < largest] or [i for i in range(1, count) if given[i] < most]
        pool, budget = sum([portions[i] for i in free]), rest
        for i in free:
            extra = min(most - given[i], max(1, budget * portions[i] // pool), rest)
            given[i] = given[i] + extra
            rest = rest - extra
    return np.array(given)


def noise(own_key, dims, scale, most, shards=(), kind=jnp.bfloat16):
    level = block_scale(own_key, dims, shards, -0.22, 0.18) if shards else 1.0
    array = jax.random.normal(own_key, dims, jnp.float32) * scale * level
    return jnp.minimum(jnp.maximum(array, -most), most).astype(kind)


def setup_inputs(seed: int = 0) -> dict:
    seeds = jax.random.split(jax.random.key(seed), 8)
    solid_start = noise(seeds[0], (NZ, NX, NY), 1.0, 6.0, ((1, 8), (2, 4)), jnp.float32)
    heat_gen = jnp.clip(0.05 * jax.random.uniform(seeds[1], (NZ, NX, NY), jnp.float32) ** block_scale(seeds[1], (NZ, NX, NY), ((1, 8), (2, 4)), -0.2, 0.2), 0.0, 0.05)
    conductance = draw_conductance(jax.random.fold_in(seeds[7], 71), 0)
    heat_capacity = jnp.clip(jnp.exp(math.log(1.0) - 1.609438 * jax.random.uniform(seeds[3], (CHANNELS,), jnp.float32) ** block_scale(seeds[3], (CHANNELS,), ((0, 4),), -0.2, 0.2)), 0.2, 1.0)
    inlet_temp = noise(seeds[4], (CHANNELS,), 1.0, 4.0, ((0, 4),), jnp.float32)
    wall_owner_keys = jax.random.split(jax.random.fold_in(seeds[5], 1), SEGS // SEG_DEV)
    wall_owner_turns = jax.random.permutation(jax.random.fold_in(seeds[5], 3), SEGS // SEG_DEV)
    wall_owner = jax.vmap(lambda own, number: deal_out(jax.random.fold_in(seeds[5], 2), own, number, SEG_DEV, N_FLOW, 1, CAP, 2))(wall_owner_keys, wall_owner_turns).reshape((SEGS, 1))
    wall_row = set_ends(jax.random.randint(seeds[6], (SEGS, 1), 0, CX), jax.random.fold_in(seeds[6], 1), 0, CX - 1).astype(jnp.int32)
    return {"solid_start": solid_start, "heat_gen": heat_gen, "conductance": conductance, "heat_capacity": heat_capacity, "inlet_temp": inlet_temp, "wall_owner": wall_owner, "wall_row": wall_row}


KAPPA = 0.16


def compose(earlier, later):
    return (earlier[0] * later[0], later[0] * earlier[1] + later[1])


def regroup(sampled_values, seg_count):
    sampled_values = sampled_values.reshape(N_FLOW, N_SPAN, CH_DEV, seg_count)
    return jnp.transpose(sampled_values, (1, 2, 0, 3)).reshape(CHANNELS, N_FLOW * seg_count)


def conduct(field, heat_gen):
    padded = jnp.pad(field, 1)
    beside = padded[2:, 1:-1, 1:-1] + padded[:-2, 1:-1, 1:-1]
    beside = beside + padded[1:-1, 2:, 1:-1] + padded[1:-1, :-2, 1:-1]
    beside = beside + padded[1:-1, 1:-1, 2:] + padded[1:-1, 1:-1, :-2]
    return field + KAPPA * (beside - 6.0 * field) + heat_gen


def reference(solid_start, heat_gen, conductance, heat_capacity, inlet_temp, wall_owner, wall_row):
    seg_count = ST_DEV // SEG
    wall_cell = regroup(wall_owner[:, 0], seg_count) * CX + regroup(wall_row[:, 0], seg_count)
    wall_cell = wall_cell.astype(jnp.int32)
    span_band = (jnp.arange(CHANNELS, dtype=jnp.int32) // CH_DEV).astype(jnp.int32)[:, None]
    decays = jnp.exp(-conductance)
    solid_field = solid_start
    coolant = jnp.zeros((CHANNELS, CHANNEL_STATIONS), jnp.float32)
    for turn in range(STEPS):
        bottom_layer = solid_field[0].reshape(NX, N_SPAN, SEG)
        wall_temp = bottom_layer[wall_cell, span_band].reshape(CHANNELS, CHANNEL_STATIONS)
        gain_pre, shift_pre = lax.associative_scan(compose, (decays, (1.0 - decays) * wall_temp), axis=1)
        coolant = gain_pre * inlet_temp[:, None] + shift_pre
        upstream = jnp.concatenate([inlet_temp[:, None], coolant[:, :-1]], axis=1)
        heat_flow = heat_capacity[:, None] * (coolant - upstream)
        wall_sink = jnp.zeros((NX, N_SPAN, SEG), jnp.float32)
        wall_sink = wall_sink.at[wall_cell, span_band].add(heat_flow.reshape(CHANNELS, N_FLOW * seg_count, SEG))
        solid_field = conduct(solid_field, heat_gen)
        solid_field = solid_field.at[0].add(-wall_sink.reshape(NX, NY))
    return solid_field, coolant
```

```python
import functools

import jax
import jax.numpy as jnp
from jax import lax
from jax.experimental import pallas as pl
from jax.experimental.pallas import tpu as pltpu
from jax.sharding import PartitionSpec as P

STEPS = 10
KAPPA = 0.16
MESH = pl.DeviceIdType.MESH
F32 = jnp.float32
BF16 = jnp.bfloat16


def split(x):
    hi = x.astype(BF16)
    lo = (x - hi.astype(F32)).astype(BF16)
    return hi, lo


def kernel(dims, cell_ref, cond_ref, lane_ref, start_ref, gen_ref, solid_out, cool_ref,
           field, ring, sides, rows_out, rows_in, cols_out, cols_in,
           decay, gain2, gain4, inner, prefix, factor, temps, own_hot, hot, seg_gain, lane_gain,
           ring_send, ring_recv, side_send, side_recv, row_send, row_recv, col_send, col_recv):
    flow, span, layers, block, seg, channels, count = dims
    width = flow * channels
    cells = flow * block
    group = 2
    me = lax.axis_index("flow")
    at = lax.axis_index("span")
    above, below = at > 0, at < span - 1
    before, after = me > 0, me < flow - 1
    levels = flow.bit_length() - 1

    def ring_copy(slot, hop):
        peer = lax.rem(me + hop, flow)
        return pltpu.make_async_remote_copy(
            src_ref=ring.at[slot, me], dst_ref=ring.at[slot, me],
            send_sem=ring_send.at[hop - 1], recv_sem=ring_recv.at[slot, hop - 1],
            device_id=(peer, at), device_id_type=MESH)

    def side_copy(slot, side):
        return pltpu.make_async_remote_copy(
            src_ref=ring.at[slot, me], dst_ref=sides.at[slot, 1 - side],
            send_sem=side_send.at[side], recv_sem=side_recv.at[slot, 1 - side],
            device_id=(me, at - 1 + 2 * side), device_id_type=MESH)

    def row_copy(slot, side):
        return pltpu.make_async_remote_copy(
            src_ref=rows_out.at[side], dst_ref=rows_in.at[slot, 1 - side],
            send_sem=row_send.at[side], recv_sem=row_recv.at[slot, 1 - side],
            device_id=(me - 1 + 2 * side, at), device_id_type=MESH)

    def col_copy(slot, side):
        return pltpu.make_async_remote_copy(
            src_ref=cols_out, dst_ref=cols_in.at[slot, 1 - side],
            send_sem=col_send.at[side], recv_sem=col_recv.at[slot, 1 - side],
            device_id=(me, at - 1 + 2 * side), device_id_type=MESH)

    def send_bottom(slot):
        for hop in range(1, flow):
            ring_copy(slot, hop).start()
        for side, there in ((0, above), (1, below)):
            @pl.when(there)
            def _():
                side_copy(slot, side).start()

    def sent_bottom(slot):
        for hop in range(1, flow):
            ring_copy(slot, hop).wait_send()
        for side, there in ((0, above), (1, below)):
            @pl.when(there)
            def _():
                side_copy(slot, side).wait_send()

    def arrived_bottom(slot):
        for hop in range(1, flow):
            ring_copy(slot, hop).wait_recv()
        for side, there in ((0, above), (1, below)):
            @pl.when(there)
            def _():
                side_copy(slot, 1 - side).wait_recv()

    def edges(act):
        for side, (in_flow, in_span) in enumerate(((before, above), (after, below))):
            @pl.when(in_flow)
            def _():
                act(row_copy, side)

            @pl.when(in_span)
            def _():
                act(col_copy, side)

    def send_edges(slot):
        edges(lambda copy, side: copy(slot, side).start())

    def sent_edges(slot):
        edges(lambda copy, side: copy(slot, side).wait_send())

    def arrived_edges(slot):
        edges(lambda copy, side: copy(slot, 1 - side).wait_recv())

    sides[...] = jnp.zeros_like(sides)
    rows_in[...] = jnp.zeros_like(rows_in)
    cols_in[...] = jnp.zeros_like(cols_in)
    barrier = pltpu.get_barrier_semaphore()
    for hop in range(1, flow):
        pl.semaphore_signal(barrier, inc=1, device_id=(lax.rem(me + hop, flow), at),
                            device_id_type=MESH)
    for side, there in ((0, above), (1, below)):
        @pl.when(there)
        def _():
            pl.semaphore_signal(barrier, inc=1, device_id=(me, at - 1 + 2 * side),
                                device_id_type=MESH)
    pl.semaphore_wait(barrier, flow - 1 + above.astype(jnp.int32) + below.astype(jnp.int32))

    lane = lax.broadcasted_iota(jnp.int32, (block, seg), 1)
    row = lax.broadcasted_iota(jnp.int32, (block, seg), 0)
    half = seg // 2

    def note_edges(z, new, marks):
        rows_out[0, pl.ds(z, 1), :] = new[0:1, :]
        rows_out[1, pl.ds(z, 1), :] = new[block - 1:block, :]
        marks = jnp.where(lane == z, new[:, 0:1], marks)
        return jnp.where(lane == half + z, new[:, seg - 1:seg], marks)

    ring[0, me] = start_ref[0]
    send_bottom(0)
    marks = jnp.zeros((block, seg), F32)
    rows_out[0, 0:1, :] = jnp.zeros((1, seg), F32)
    rows_out[1, 0:1, :] = jnp.zeros((1, seg), F32)
    field[0, layers] = jnp.zeros((block, seg), F32)
    field[1, layers] = jnp.zeros((block, seg), F32)
    for z in range(1, layers):
        new = start_ref[z]
        field[0, z] = new
        marks = note_edges(z, new, marks)
    cols_out[...] = marks
    send_edges(0)

    nwide = group * width
    place = lax.rem(lax.broadcasted_iota(jnp.int32, (seg, nwide), 0), 8)
    near1, near2, near4 = place >= 1, place >= 2, place >= 4

    def turned(x, k):
        return pltpu.roll(x.reshape(seg // 8, 8, nwide), k, 1).reshape(seg, nwide)

    for pair in range(count // group):
        span_of = pl.ds(pair * nwide, nwide)
        cond = cond_ref[:, span_of]
        d = jnp.exp(-cond)
        decay[:, span_of] = d
        capacity = jnp.concatenate([lane_ref[0:1, :]] * group, axis=1)
        factor[:, span_of] = (jnp.exp(cond) - 1.0) * capacity
        g1 = d * jnp.where(near1, turned(d, 1), 1.0)
        gain2[:, span_of] = jnp.where(near2, g1, 0.0)
        g2 = g1 * jnp.where(near2, turned(g1, 2), 1.0)
        gain4[:, span_of] = jnp.where(near4, g2, 0.0)
        g3 = g2 * jnp.where(near4, turned(g2, 4), 1.0)
        inner[:, span_of] = g3
        enter = jnp.ones((1, nwide), F32)
        for g in range(seg // 8):
            here = g3[8 * g:8 * g + 8] * enter
            prefix[8 * g:8 * g + 8, span_of] = here
            enter = here[7:8]
        target = cell_ref[0:1, span_of]
        mine = target - (me * block).astype(F32)
        own_hot[:, span_of] = (
            lax.broadcasted_iota(jnp.int32, (block, nwide), 0).astype(F32) == mine).astype(BF16)
        if hot is not None:
            hot[:, span_of] = (
                lax.broadcasted_iota(jnp.int32, (cells, nwide), 0).astype(F32) == target
            ).astype(BF16)

    gain = jnp.ones((1, width), F32)
    for t in range(count):
        seg_gain[t:t + 1, :] = gain
        gain = gain * prefix[seg - 1:seg, t * width:(t + 1) * width]
    number = lax.broadcasted_iota(jnp.int32, (1, width), 1) // channels
    for level in range(levels):
        far = number >= (1 << level)
        lane_gain[level:level + 1, :] = jnp.where(far, gain, 0.0)
        gain = gain * jnp.where(far, pltpu.roll(jnp.broadcast_to(gain, (8, width)), channels << level, 1)[0:1], 1.0)
    upper = jnp.where(number >= 1, pltpu.roll(jnp.broadcast_to(gain, (8, width)), channels, 1)[0:1], 1.0)
    lane_gain[levels:levels + 1, :] = upper * lane_ref[1:2, :]

    def roll_lanes(x, k):
        return pltpu.roll(jnp.broadcast_to(x, (8, width)), k, 1)[0:1]

    def around(c, low_row, high_row, low_col, high_col):
        beside = jnp.where(row == 0, low_row, pltpu.roll(c, 1, 0))
        beside = beside + jnp.where(row == block - 1, high_row, pltpu.roll(c, block - 1, 0))
        beside = beside + jnp.where(lane == 0, low_col, pltpu.roll(c, 1, 1))
        return beside + jnp.where(lane == seg - 1, high_col, pltpu.roll(c, seg - 1, 1))

    def step(turn, carry):
        slot, later = lax.rem(turn, 2), lax.rem(turn + 1, 2)
        arrived_bottom(slot)
        sent_bottom(slot)
        base = ring[slot].reshape(cells, seg)
        hi, lo = split(base.T)
        lhs = jnp.concatenate([hi, lo], axis=0)
        for pair in range(count // group):
            span_of = pl.ds(pair * nwide, nwide)
            if hot is not None:
                picked = jnp.dot(lhs, hot[:, span_of], preferred_element_type=F32)
            else:
                picked = jnp.zeros((2 * seg, nwide), F32)
                part = min(cells, 512)
                for first in range(0, cells, part):
                    one = (lax.broadcasted_iota(jnp.int32, (part, nwide), 0) + first).astype(F32)
                    one = (one == cell_ref[0:1, span_of]).astype(BF16)
                    picked += jnp.dot(lhs[:, first:first + part], one, preferred_element_type=F32)
            w = picked[:seg] + picked[seg:]
            temps[:, span_of] = w
            d = decay[:, span_of]
            s = w - d * w
            s = s + jnp.where(near1, d, 0.0) * turned(s, 1)
            s = s + gain2[:, span_of] * turned(s, 2)
            s = s + gain4[:, span_of] * turned(s, 4)
            cool_ref[:, span_of] = s
        for t in range(count):
            span_of = pl.ds(t * width, width)
            enter = jnp.zeros((1, width), F32)
            for g in range(seg // 8):
                here = pl.ds(8 * g, 8)
                local = cool_ref[here, span_of]
                if g:
                    local = local + inner[here, span_of] * enter
                    cool_ref[here, span_of] = local
                enter = local[7:8]
        run = jnp.zeros((1, width), F32)
        runs = []
        for t in range(count):
            runs.append(run)
            whole = pl.ds(t * width, width)
            run = prefix[seg - 1:seg, whole] * run + cool_ref[seg - 1:seg, whole]
        for level in range(levels):
            run = run + lane_gain[level:level + 1, :] * roll_lanes(run, channels << level)
        carry_in = jnp.where(number >= 1, roll_lanes(run, channels), 0.0) + lane_gain[levels:levels + 1, :]
        sink = jnp.zeros((block, 2 * seg), F32)
        for pair in range(count // group):
            span_of = pl.ds(pair * nwide, nwide)
            enter = jnp.concatenate(
                [runs[t] + seg_gain[t:t + 1, :] * carry_in
                 for t in range(pair * group, (pair + 1) * group)], axis=1)
            coolant = cool_ref[:, span_of] + prefix[:, span_of] * enter
            cool_ref[:, span_of] = coolant
            heat = factor[:, span_of] * (temps[:, span_of] - coolant)
            hi, lo = split(heat)
            sink = sink + lax.dot_general(
                own_hot[:, span_of], jnp.concatenate([hi, lo], axis=0),
                (((1,), (1,)), ((), ())), preferred_element_type=F32)
        sink = sink[:, :seg] + sink[:, seg:]
        c = ring[slot, me]
        low = ring[slot, jnp.maximum(me - 1, 0), block - 1:block, :]
        high = ring[slot, jnp.minimum(me + 1, flow - 1), 0:1, :]
        low = jnp.where(before, low, 0.0)
        high = jnp.where(after, high, 0.0)
        beside = around(c, low, high, sides[slot, 0][:, seg - 1:seg], sides[slot, 1][:, 0:1])
        beside = beside + field[slot, 1]
        bottom = c + KAPPA * (beside - 6.0 * c) + gen_ref[0] - sink
        ring[later, me] = bottom
        solid_out[0] = bottom

        @pl.when(turn < STEPS - 1)
        def _():
            send_bottom(later)

        arrived_edges(slot)
        sent_edges(slot)
        marks = jnp.zeros((block, seg), F32)
        low_cols = cols_in[slot, 0]
        high_cols = cols_in[slot, 1]
        for z in range(1, layers):
            c = field[slot, z]
            beside = around(c, rows_in[slot, 0, z:z + 1, :], rows_in[slot, 1, z:z + 1, :],
                            low_cols[:, half + z:half + z + 1], high_cols[:, z:z + 1])
            under = ring[slot, me] if z == 1 else field[slot, z - 1]
            beside = beside + under + field[slot, z + 1]
            new = c + KAPPA * (beside - 6.0 * c) + gen_ref[z]
            field[later, z] = new
            marks = note_edges(z, new, marks)
        cols_out[...] = marks

        @pl.when(turn < STEPS - 1)
        def _():
            send_edges(later)
        return carry

    lax.fori_loop(0, STEPS, step, 0)
    last = STEPS % 2
    for z in range(1, layers):
        solid_out[z] = field[last, z]


def body(solid_start, heat_gen, conductance, heat_capacity, inlet_temp, wall_owner, wall_row):
    flow = lax.axis_size("flow")
    span = lax.axis_size("span")
    layers, block, seg = solid_start.shape
    channels, stations = conductance.shape
    count = stations // seg
    segs = channels * count
    me = lax.axis_index("flow")
    cell = (wall_owner[:, 0] * block + wall_row[:, 0]).astype(F32).reshape(segs // seg, seg)
    packed = jnp.concatenate([conductance.reshape(segs, seg), cell], axis=0)
    packed = lax.all_gather(packed, "flow")
    cond = packed[:, :segs].reshape(flow, channels, count, seg)
    cond = jnp.transpose(cond, (3, 2, 0, 1)).reshape(seg, count * flow * channels)
    cell = packed[:, segs:].reshape(flow, channels, count)
    cell = jnp.transpose(cell, (2, 0, 1)).reshape(1, count * flow * channels)
    per_lane = jnp.stack([jnp.tile(heat_capacity, flow), jnp.tile(inlet_temp, flow)])
    width = flow * channels
    total = count * width
    keep = flow * block * total * 2 <= (8 << 20)
    dims = (flow, span, layers, block, seg, channels, count)
    vm = pltpu.VMEM
    dma = pltpu.SemaphoreType.DMA
    big = vm((seg, total), F32)
    scratch = [
        vm((2, layers + 1, block, seg), F32), vm((2, flow, block, seg), F32),
        vm((2, 2, block, seg), F32), vm((2, layers, seg), F32), vm((2, 2, layers, seg), F32),
        vm((block, seg), F32), vm((2, 2, block, seg), F32),
        big, big, big, big, big, big, big, vm((block, total), BF16),
    ]
    if keep:
        scratch.append(vm((flow * block, total), BF16))
    scratch += [
        vm((count, width), F32), vm((8, width), F32),
        dma((flow - 1,)), dma((2, flow - 1)), dma((2,)), dma((2, 2)),
        dma((2,)), dma((2, 2)), dma((2,)), dma((2, 2)),
    ]

    def run(*refs):
        if not keep:
            refs = refs[:22] + (None,) + refs[22:]
        kernel(dims, *refs)

    solid, cool = pl.pallas_call(
        run,
        out_shape=(jax.ShapeDtypeStruct(solid_start.shape, F32),
                   jax.ShapeDtypeStruct((seg, total), F32)),
        in_specs=[pl.BlockSpec(memory_space=pltpu.VMEM)] * 5,
        out_specs=(pl.BlockSpec(memory_space=pltpu.VMEM),) * 2,
        scratch_shapes=scratch,
        compiler_params=pltpu.CompilerParams(
            collective_id=0, has_side_effects=True, vmem_limit_bytes=60 << 20),
    )(cell, cond, per_lane, solid_start, heat_gen)
    cool = cool.reshape(seg, count, flow, channels)
    cool = lax.dynamic_index_in_dim(cool, me, 2, False)
    return solid, jnp.transpose(cool, (2, 1, 0)).reshape(channels, stations)


def solution(mesh):
    placed = (
        P(None, "flow", "span"),
        P(None, "flow", "span"),
        P("span", "flow"),
        P("span"),
        P("span"),
        P(("flow", "span"), None),
        P(("flow", "span"), None),
    )
    return jax.shard_map(
        body,
        mesh=mesh,
        in_specs=placed,
        out_specs=(P(None, "flow", "span"), P("span", "flow")),
        check_vma=False,
    )
```
